32 devices in a mesh: seq: 8 (over z, core), cp: 4 (over y, x).
Axes of the slice: x: 2, y: 2, z: 4, core: 2. Of those that a mesh axis runs over, the one named last changes fastest.
Arguments:
- queries: bfloat16 [4096, 768], P(('seq', 'cp')), parts along dimension 0, may hold values from -6 to 6, as said below
- keys: bfloat16 [4096, 128], P(('seq', 'cp')), parts along dimension 0, may hold values from -6 to 6, as said below
- values: bfloat16 [4096, 128], P(('seq', 'cp')), parts along dimension 0, may hold values from -6 to 6
- out_grad: bfloat16 [4096, 768], P(('seq', 'cp')), parts along dimension 0, may hold values from -6 to 6
- positions: int32 [3, 4096], P(None, 'seq'), parts along dimension 1, may hold values from 0 to 511
- doc_ids: int32 [4096], P('seq'), parts along dimension 0, may hold values from 0 to 7, never falling along the last dimension, each value on 1 to 256 neighbouring positions
- stretch_order: int32 [64], P('seq'), parts along dimension 0, may hold values from 0 to 7, each once
Outputs:
- attn_out: bfloat16 [4096, 768], P(('seq', 'cp')), parts along dimension 0
- grad_queries: bfloat16 [4096, 768], P(('seq', 'cp')), parts along dimension 0
- grad_keys: bfloat16 [4096, 128], P(('seq', 'cp')), parts along dimension 0
- grad_values: bfloat16 [4096, 128], P(('seq', 'cp')), parts along dimension 0
The draws below stay inside these ranges and needn't reach their ends.
There are 8 independent parts, one for each index of `seq`. The reference program is written for one: setup_inputs(seed, part) draws one part's arguments, and reference() takes and returns one part's arrays. A program takes and returns all parts, laid end to end along the dimension named above; each array names one. Nothing has to cross between parts.
Inputs may be any that keep to these rules, and one draw needn't show every extreme that they name: `queries`: values of one part; a few tokens may have large entries. `keys`: values of one part; a few tokens may have large entries. `doc_ids`: never falls along the sequence; each document holds at most 256 tokens. `stretch_order`: each block number appears once.
All inputs are finite; a program needn't handle non-finite values.
Results may differ from the reference program's by a relative error of at most 0.01.
Values may be sent and summed in bfloat16 or wider, within the bound.
A program may use at most 64 MiB of HBM per device.

```python
import math
import jax
import jax.numpy as jnp
import numpy as np
from jax import lax

HQ = 6
HK = 1
HD = 128
DOCS = 8
GROUP = 6
SEC_T = 16
SEC_H = 24
STRETCH = 64
STRETCHES = 8
SEQ_LEN = 512


def draw_keys(key, part):
    base = jnp.clip(jax.random.normal(jax.random.fold_in(key, 1), (SEQ_LEN, HK * HD)), -6.0, 6.0)
    return base.astype(jnp.bfloat16)


def draw_queries(key, part):
    base = jnp.clip(jax.random.normal(jax.random.fold_in(key, 2), (SEQ_LEN, HQ * HD)), -6.0, 6.0)
    return base.astype(jnp.bfloat16)


def set_ends(entries, stream_key, low, high):
    place = [jax.random.randint(jax.random.fold_in(stream_key, axis), (), 0, length) for axis, length in enumerate(entries.shape)]
    main_axis = entries.shape.index(max(entries.shape))
    next_to = place[:main_axis] + [(place[main_axis] + 1) % entries.shape[main_axis]] + place[main_axis + 1:]
    return entries.at[tuple(place)].set(low).at[tuple(next_to)].set(high)


def block_levels(rng, shape, shards, smallest, largest):
    loudness = 1.0
    for dim, blocks in shards:
        steps = jax.random.uniform(jax.random.fold_in(jax.random.fold_in(rng, 6), dim), (blocks,), jnp.float32, smallest / len(shards), largest / len(shards))
        loudness = loudness * jnp.repeat(jnp.exp(steps), shape[dim] // blocks).reshape((-1,) + (1,) * (len(shape) - 1 - dim))
    return loudness


def length_profile(amount, total, bound, slope):
    weights = [(1 << 20) // math.isqrt(grade ** slope) + 1 for grade in range(2, amount + 1)]
    spare, given = total - bound - (amount - 1), [1] * (amount - 1)
    while spare > 0:
        candidates = [i for i in range(amount - 1) if given[i] < bound]
        mass, budget = sum([weights[i] for i in candidates]), spare
        for i in candidates:
            addition = min(bound - given[i], max(1, budget * weights[i] // mass), spare)
            given[i] = given[i] + addition
            spare = spare - addition
    return np.array([bound] + given)


def ragged_sizes(stream_key, number_of, total, bound, skew):
    if number_of == 2:
        one = jax.random.randint(stream_key, (), max(1, total - bound), min(bound, total - 1) + 1)
        return jnp.stack([one, total - one])
    sizes = jnp.asarray(length_profile(number_of, total, bound, skew), jnp.int32)
    pairs = (number_of - 1) // 2
    donor, sink = sizes[1:1 + 2 * pairs:2], sizes[2:2 + 2 * pairs:2]
    margin = jnp.minimum(donor - 1, bound - sink)
    shifted = jax.random.randint(jax.random.fold_in(stream_key, 1), (pairs,), 0, 1 << 20) % (margin + 1)
    sizes = sizes.at[1:1 + 2 * pairs:2].set(donor - shifted).at[2:2 + 2 * pairs:2].set(sink + shifted)
    return sizes[jax.random.permutation(jax.random.fold_in(stream_key, 2), number_of)]


def normal_values(own_key, extent, deviation, most, split=(), kind=jnp.bfloat16):
    loudness = block_levels(own_key, extent, split, -0.22, 0.18) if split else 1.0
    values = jax.random.normal(own_key, extent, jnp.float32) * deviation * loudness
    return jnp.minimum(jnp.maximum(values, -most), most).astype(kind)


def setup_inputs(seed: int = 0, part: int = 0) -> dict:
    arg_keys = jax.random.split(jax.random.key(seed), 8)
    part_keys = jax.random.split(jax.random.fold_in(arg_keys[7], part), 8)
    queries = draw_queries(jax.random.fold_in(jax.random.fold_in(arg_keys[7], part), 71), part)
    keys = draw_keys(jax.random.fold_in(jax.random.fold_in(arg_keys[7], part), 71), part)
    values = normal_values(part_keys[2], (SEQ_LEN, HK * HD), 1.0, 6.0, ((0, 4),))
    out_grad = normal_values(part_keys[3], (SEQ_LEN, HQ * HD), 1.0, 6.0, ((0, 4),))
    positions = set_ends(jax.random.randint(part_keys[4], (3, SEQ_LEN), 0, SEQ_LEN), jax.random.fold_in(part_keys[4], 1), 0, SEQ_LEN - 1).astype(jnp.int32)
    doc_ids = jnp.searchsorted(jnp.cumsum(ragged_sizes(part_keys[5], DOCS, SEQ_LEN, SEQ_LEN // 2, 2)), jnp.arange(SEQ_LEN), side="right").astype(jnp.int32)
    stretch_order = jax.random.permutation(part_keys[6], STRETCHES).astype(jnp.int32)
    return {"queries": queries, "keys": keys, "values": values, "out_grad": out_grad, "positions": positions, "doc_ids": doc_ids, "stretch_order": stretch_order}


def rotary_tables(pos3):
    half = HD // 2
    pairs = jnp.arange(half, dtype=jnp.int32)
    freqs = jnp.exp(-(2.0 * pairs.astype(jnp.float32) / HD) * math.log(1000000.0))
    pos_f = pos3.astype(jnp.float32)
    chosen = jnp.where((pairs < SEC_T)[None, :], pos_f[0][:, None], jnp.where((pairs < SEC_T + SEC_H)[None, :], pos_f[1][:, None], pos_f[2][:, None]))
    angle = chosen * freqs[None, :]
    cosine = jnp.concatenate([jnp.cos(angle), jnp.cos(angle)], axis=1)
    sine_tab = jnp.concatenate([jnp.sin(angle), jnp.sin(angle)], axis=1)
    return (cosine, sine_tab)

def rotate(field, cosine, sine_tab):
    half = HD // 2
    first, second = (field[..., :half], field[..., half:])
    turned = jnp.concatenate([-second, first], axis=-1)
    return field * cosine[:, None, :] + turned * sine_tab[:, None, :]

def rotate_back(field, cosine, sine_tab):
    half = HD // 2
    scaled = field * sine_tab[:, None, :]
    turned = jnp.concatenate([scaled[..., half:], -scaled[..., :half]], axis=-1)
    return field * cosine[:, None, :] + turned

def reference(queries, keys, values, out_grad, positions, doc_ids, stretch_order):
    length = SEQ_LEN
    orig = (stretch_order[:, None] * STRETCH + jnp.arange(STRETCH, dtype=jnp.int32)[None, :]).reshape(length)
    docs = doc_ids[orig]
    cosine, sine_tab = rotary_tables(positions[:, orig])
    q_rot = rotate(queries.astype(jnp.float32).reshape(length, HQ, HD), cosine, sine_tab).astype(jnp.bfloat16)
    k_rot = rotate(keys.astype(jnp.float32).reshape(length, HK, HD), cosine, sine_tab).astype(jnp.bfloat16)
    val_heads = values.reshape(length, HK, HD)
    grad_heads = out_grad.reshape(length, HQ, HD)
    allowed = (docs[:, None] == docs[None, :]) & (orig[None, :] <= orig[:, None])
    score_scale = 1.0 / math.sqrt(HD)
    outputs, dq_list, dk_list, dv_list = ([], [], [], [])
    for group_id in range(HK):
        q_grp = q_rot[:, group_id * GROUP:(group_id + 1) * GROUP, :].astype(jnp.float32)
        k_grp = k_rot[:, group_id, :].astype(jnp.float32)
        v_grp = val_heads[:, group_id, :].astype(jnp.float32)
        do_grp = grad_heads[:, group_id * GROUP:(group_id + 1) * GROUP, :].astype(jnp.float32)
        scores = jnp.einsum('tgd,kd->tgk', q_grp, k_grp) * score_scale
        scores = jnp.where(allowed[:, None, :], scores, -jnp.inf)
        top = lax.optimization_barrier(jnp.max(scores, axis=-1, keepdims=True))
        expo = jnp.exp(scores - top)
        probs32 = expo / lax.optimization_barrier(jnp.sum(expo, axis=-1, keepdims=True))
        probs = probs32.astype(jnp.bfloat16)
        outputs.append(jnp.einsum('tgk,kd->tgd', probs.astype(jnp.float32), v_grp).astype(jnp.bfloat16))
        dprobs = jnp.einsum('tgd,kd->tgk', do_grp, v_grp)
        delta = lax.optimization_barrier(jnp.sum(probs32 * dprobs, axis=-1, keepdims=True))
        dscores = (probs32 * (dprobs - delta)).astype(jnp.bfloat16).astype(jnp.float32)
        dq_list.append(jnp.einsum('tgk,kd->tgd', dscores, k_grp) * score_scale)
        dk_list.append(jnp.einsum('tgk,tgd->kd', dscores, q_grp) * score_scale)
        dv_list.append(jnp.einsum('tgk,tgd->kd', probs.astype(jnp.float32), do_grp))
    attn_out = jnp.concatenate(outputs, axis=1).reshape(length, HQ * HD)
    dq_rot = jnp.concatenate(dq_list, axis=1)
    dk_rot = jnp.stack(dk_list, axis=1)
    grad_queries = rotate_back(dq_rot, cosine, sine_tab).astype(jnp.bfloat16).reshape(length, HQ * HD)
    grad_keys = rotate_back(dk_rot, cosine, sine_tab).astype(jnp.bfloat16).reshape(length, HK * HD)
    grad_values = jnp.stack(dv_list, axis=1).astype(jnp.bfloat16).reshape(length, HK * HD)
    return (attn_out, grad_queries, grad_keys, grad_values)
```

```python
import functools
import math

import jax
import jax.numpy as jnp
from jax import lax
from jax.experimental import pallas as pl
from jax.experimental.pallas import tpu as pltpu
from jax.sharding import PartitionSpec as P

HQ = 6
HD = 128
SEC_T = 16
SEC_H = 24
BASE = 1000000.0
NEG = -1e30
F32 = jnp.float32
BF16 = jnp.bfloat16


def nt(a, b):
    return lax.dot_general(a, b, (((1,), (1,)), ((), ())), preferred_element_type=F32)


def nn(a, b):
    return lax.dot_general(a, b, (((1,), (0,)), ((), ())), preferred_element_type=F32)


def cos_turns(turns):
    r = turns - jnp.round(turns)
    b = 0.25 - jnp.abs(r)
    z = b * b
    acc = None
    for power in (11, 9, 7, 5, 3, 1):
        coef = (-1.0) ** ((power - 1) // 2) * (2.0 * math.pi) ** power / math.factorial(power)
        acc = jnp.full_like(z, coef) if acc is None else acc * z + coef
    return acc * b


def flip(me, i):
    out, bit = me, 1
    while bit <= i:
        if i & bit:
            out = out + bit - 2 * bit * ((me // bit) % 2)
        bit *= 2
    return out


def repeat(n, small, body):
    if small:
        for i in range(n):
            body(i)
    else:
        lax.fori_loop(0, n, lambda i, c: (body(i), c)[1], 0)


def kernel(n, order_ref, q_hbm, k_hbm, v_hbm, do_hbm, pos_hbm, doc_hbm,
           out_ref, gq_ref, gk_ref, gv_ref,
           q_in, do_in, pos_in, doc_in, k_all, v_all, feat, lay, seqtab, q_rot, do_st, krot,
           cos_t, sin_t, s_buf, dp_buf, p_buf, ds_buf, send_buf, recv_buf,
           in_sem, ks_sem, kr_sem, vs_sem, vr_sem, gs_sem, gr_sem):
    me = lax.axis_index("cp")
    rows = k_hbm.shape[0]
    total = rows * n
    stretch = total // order_ref.shape[0]
    per = rows // stretch
    small = n <= 4 and n & (n - 1) == 0
    scale = 1.0 / math.sqrt(HD)
    mine = pl.ds(pl.multiple_of(me * rows, rows), rows)

    def to(i):
        return flip(me, i) if small else lax.rem(me + i, n)

    def frm(i):
        return flip(me, i) if small else lax.rem(me + n - i, n)

    def span(c):
        return pl.ds(pl.multiple_of(c * rows, rows), rows)

    loads = [
        pltpu.make_async_copy(src, dst, in_sem.at[j])
        for j, (src, dst) in enumerate((
            (k_hbm, k_all.at[mine]), (v_hbm, v_all.at[mine]), (pos_hbm, pos_in),
            (doc_hbm, doc_in), (q_hbm, q_in), (do_hbm, do_in)))
    ]
    for cp in loads:
        cp.start()

    barrier = pltpu.get_barrier_semaphore()

    def greet(i):
        pl.semaphore_signal(barrier, inc=1, device_id={"cp": to(i + 1)},
                            device_id_type=pl.DeviceIdType.MESH)

    repeat(n - 1, small, greet)
    loads[0].wait()
    loads[1].wait()
    pl.semaphore_wait(barrier, n - 1)

    def kcopy(i):
        return pltpu.make_async_remote_copy(
            src_ref=k_all.at[mine], dst_ref=k_all.at[mine], send_sem=ks_sem.at[i],
            recv_sem=kr_sem.at[i], device_id={"cp": to(i)}, device_id_type=pl.DeviceIdType.MESH)

    def vcopy(i):
        return pltpu.make_async_remote_copy(
            src_ref=v_all.at[mine], dst_ref=v_all.at[mine], send_sem=vs_sem.at[i],
            recv_sem=vr_sem.at[i], device_id={"cp": to(i)}, device_id_type=pl.DeviceIdType.MESH)

    repeat(n - 1, small, lambda i: kcopy(n - 1 - i).start())
    repeat(n - 1, small, lambda i: vcopy(n - 1 - i).start())

    for j in (2, 3):
        loads[j].wait()
    feat[...] = jnp.zeros_like(feat)
    feat[0:3, :] = pos_in[...].astype(F32)
    feat[3:4, :] = doc_in[...].astype(F32)
    tiles = [feat[:, t * rows:(t + 1) * rows] for t in range(n)]
    moved = [[tiles[t] if k == 0 else pltpu.roll(tiles[t], k * stretch, 1) for k in range(per)]
             for t in range(n)]
    lane8 = lax.broadcasted_iota(jnp.int32, (8, rows), 1)
    for t in range(n):
        whole = None
        for b in range(per):
            want = jnp.full((8, rows), order_ref[t * per + b], jnp.int32)
            acc = moved[0][b]
            for s in range(1, n * per):
                acc = jnp.where(want == s, moved[s // per][(b - s % per) % per], acc)
            whole = acc if b == 0 else jnp.where(lane8 >= b * stretch, acc, whole)
        lay[:, t * rows:(t + 1) * rows] = whole
    lane = lax.broadcasted_iota(jnp.int32, (8, 2 * HD), 1)
    row8 = lax.broadcasted_iota(jnp.int32, (8, 2 * HD), 0)
    pair = lane % (HD // 2)
    section = jnp.where(pair < SEC_T, 0, jnp.where(pair < SEC_T + SEC_H, 1, 2))
    freq = jnp.exp(pair.astype(F32) * (-2.0 / HD * math.log(BASE))) * (0.5 / math.pi)
    weights = jnp.where(lane < HD, jnp.where(row8 == section, freq, 0.0),
                        jnp.where(row8 == 3, 1.0, 0.0))
    seqtab[...] = lax.dot_general(lay[...], weights, (((0,), (0,)), ((), ())),
                                  precision=lax.Precision.HIGHEST, preferred_element_type=F32)

    first = lax.broadcasted_iota(jnp.int32, (rows, HD), 1) < HD // 2

    def blocks(c):
        return seqtab[span(c), :]

    def tables(turns):
        both = cos_turns(jnp.where(first, turns, turns - 0.25))
        other = pltpu.roll(both, HD // 2, 1)
        return jnp.where(first, both, other), jnp.where(first, -other, both)

    def turned(x):
        return pltpu.roll(x, HD // 2, 1)

    own = blocks(me)
    cosine, sine = tables(own[:, :HD])
    cos_t[...] = cosine
    sin_t[...] = sine
    r_idx = lax.broadcasted_iota(jnp.int32, (rows, HD), 0)
    l_idx = lax.broadcasted_iota(jnp.int32, (rows, HD), 1)
    doc_r = lay[3:4, mine]

    def places(c, idx):
        out = idx + order_ref[c * per] * stretch
        for b in range(1, per):
            out = jnp.where(idx >= b * stretch,
                            idx - b * stretch + order_ref[c * per + b] * stretch, out)
        return out

    orig_r = places(me, l_idx)

    loads[4].wait()
    loads[5].wait()
    for h in range(HQ):
        x = q_in[:, h * HD:(h + 1) * HD].astype(F32)
        q_rot[h * rows:(h + 1) * rows, :] = (x * cosine + turned(x) * sine).astype(BF16)
        do_st[h * rows:(h + 1) * rows, :] = do_in[:, h * HD:(h + 1) * HD]

    def chunk(c, tab, cc, ss, top):
        allowed = (tab[:, HD:] == doc_r) & (places(c, r_idx) <= orig_r)
        bias = jnp.where(allowed, 0.0, NEG)
        x = k_all[span(c), :].astype(F32)
        kr = (x * cc + turned(x) * ss).astype(BF16)
        krot[span(c), :] = kr
        sc = nt(kr, q_rot[...])
        tops = []
        for h in range(HQ):
            part = sc[:, h * HD:(h + 1) * HD] + bias
            s_buf[span(c), h * HD:(h + 1) * HD] = part
            tops.append(jnp.max(part, axis=0, keepdims=True))
        return jnp.maximum(top, jnp.concatenate(tops, axis=1))

    def grads(c):
        dp_buf[span(c), :] = nt(v_all[span(c), :], do_st[...])

    top = jnp.full((1, HQ * rows), NEG, F32)
    top = chunk(me, own, cosine, sine, top)
    grads(me)

    def arrive(i, top):
        c = frm(i)
        tab = blocks(c)
        cc, ss = tables(tab[:, :HD])
        kcopy(i).wait_recv()
        top = chunk(c, tab, cc, ss, top)
        vcopy(i).wait_recv()
        grads(c)
        return top

    if small:
        for i in range(1, n):
            top = arrive(i, top)
    else:
        top = lax.fori_loop(1, n, arrive, top)

    factor = scale * math.log2(math.e)

    def soft(c, carry):
        total_p, total_d = carry
        p = jnp.exp2((s_buf[span(c), :] - top) * factor)
        s_buf[span(c), :] = p
        return (total_p + jnp.sum(p, axis=0, keepdims=True),
                total_d + jnp.sum(p * dp_buf[span(c), :], axis=0, keepdims=True))

    zero = jnp.zeros((1, HQ * rows), F32)
    carry = (zero, zero)
    if small:
        for c in range(n):
            carry = soft(c, carry)
    else:
        carry = lax.fori_loop(0, n, soft, carry)
    inv = 1.0 / carry[0]
    delta = carry[1] * inv

    def back(c):
        probs = s_buf[span(c), :] * inv
        pb = probs.astype(BF16)
        db = (probs * (dp_buf[span(c), :] - delta)).astype(BF16)
        p_buf[span(c), :] = pb
        ds_buf[span(c), :] = db
        return nn(db, q_rot[...]) * scale, nn(pb, do_st[...])

    def gcopy(i):
        return pltpu.make_async_remote_copy(
            src_ref=send_buf.at[i - 1], dst_ref=recv_buf.at[i - 1], send_sem=gs_sem.at[i],
            recv_sem=gr_sem.at[i], device_id={"cp": to(i)}, device_id_type=pl.DeviceIdType.MESH)

    def give(j):
        i = n - 1 - j
        dk, dv = back(to(i))
        send_buf[i - 1, :, :HD] = dk.astype(BF16)
        send_buf[i - 1, :, HD:] = dv.astype(BF16)
        gcopy(i).start()

    repeat(n - 1, small, give)
    dk, dv = back(me)

    outt = lax.dot_general(v_all[...], p_buf[...], (((0,), (0,)), ((), ())),
                           preferred_element_type=F32)
    dqt = lax.dot_general(krot[...], ds_buf[...], (((0,), (0,)), ((), ())),
                          preferred_element_type=F32) * scale
    for h in range(HQ):
        cols = slice(h * HD, (h + 1) * HD)
        out_ref[:, cols] = jnp.transpose(outt[:, h * rows:(h + 1) * rows]).astype(BF16)
        y = jnp.transpose(dqt[:, h * rows:(h + 1) * rows])
        gq_ref[:, cols] = (y * cos_t[...] - turned(y) * sin_t[...]).astype(BF16)

    def take(i, carry):
        gcopy(i).wait_recv()
        return (carry[0] + recv_buf[i - 1, :, :HD].astype(F32),
                carry[1] + recv_buf[i - 1, :, HD:].astype(F32))

    if small:
        for i in range(1, n):
            dk, dv = take(i, (dk, dv))
    else:
        dk, dv = lax.fori_loop(1, n, take, (dk, dv))
    gk_ref[...] = (dk * cos_t[...] - turned(dk) * sin_t[...]).astype(BF16)
    gv_ref[...] = dv.astype(BF16)

    def finish(j):
        kcopy(j + 1).wait_send()
        vcopy(j + 1).wait_send()
        gcopy(j + 1).wait_send()

    repeat(n - 1, small, finish)


def write_out(a, b, c, d, a_out, b_out, c_out, d_out, sem):
    copies = [
        pltpu.make_async_copy(src, dst, sem.at[j])
        for j, (src, dst) in enumerate(((a, a_out), (b, b_out), (c, c_out), (d, d_out)))
    ]
    for cp in copies:
        cp.start()
    for cp in copies:
        cp.wait()


def shards(queries, keys, values, out_grad, positions, doc_ids, stretch_order):
    n = lax.axis_size("cp")
    rows = queries.shape[0]
    total = rows * n
    wide = HQ * HD
    hbm = pl.BlockSpec(memory_space=pltpu.HBM)
    vmem = pl.BlockSpec(memory_space=pltpu.VMEM)
    dma = pltpu.SemaphoreType.DMA
    shapes = ((rows, wide), (rows, wide), (rows, HD), (rows, HD))
    held = pl.pallas_call(
        functools.partial(kernel, n),
        out_shape=tuple(pltpu.VMEM(shape, BF16) for shape in shapes),
        in_specs=[pl.BlockSpec(memory_space=pltpu.SMEM)] + [hbm] * 6,
        out_specs=(vmem,) * 4,
        scratch_shapes=[
            pltpu.VMEM((rows, wide), BF16),
            pltpu.VMEM((rows, wide), BF16),
            pltpu.VMEM((3, total), jnp.int32),
            pltpu.VMEM((1, total), jnp.int32),
            pltpu.VMEM((total, HD), BF16),
            pltpu.VMEM((total, HD), BF16),
            pltpu.VMEM((8, total), F32),
            pltpu.VMEM((8, total), F32),
            pltpu.VMEM((total, 2 * HD), F32),
            pltpu.VMEM((HQ * rows, HD), BF16),
            pltpu.VMEM((HQ * rows, HD), BF16),
            pltpu.VMEM((total, HD), BF16),
            pltpu.VMEM((rows, HD), F32),
            pltpu.VMEM((rows, HD), F32),
            pltpu.VMEM((total, HQ * rows), F32),
            pltpu.VMEM((total, HQ * rows), F32),
            pltpu.VMEM((total, HQ * rows), BF16),
            pltpu.VMEM((total, HQ * rows), BF16),
            pltpu.VMEM((n - 1, rows, 2 * HD), BF16),
            pltpu.VMEM((n - 1, rows, 2 * HD), BF16),
            dma((6,)),
            dma((n,)), dma((n,)), dma((n,)), dma((n,)), dma((n,)), dma((n,)),
        ],
        compiler_params=pltpu.CompilerParams(collective_id=0, has_side_effects=True),
    )(stretch_order, queries, keys, values, out_grad, positions, doc_ids[None, :])
    return pl.pallas_call(
        write_out,
        out_shape=tuple(jax.ShapeDtypeStruct(shape, BF16) for shape in shapes),
        in_specs=[vmem] * 4,
        out_specs=(hbm,) * 4,
        scratch_shapes=[dma((4,))],
    )(*[pltpu.with_memory_space_constraint(x, pltpu.VMEM) for x in held])


def solution(mesh):
    split = P(("seq", "cp"), None)
    return jax.shard_map(
        shards,
        mesh=mesh,
        in_specs=(split, split, split, split, P(None, "seq"), P("seq"), P("seq")),
        out_specs=(split, split, split, split),
        check_vma=False,
    )
```

```python
import functools
import math

import jax
import jax.numpy as jnp
from jax import lax
from jax.experimental import pallas as pl
from jax.experimental.pallas import tpu as pltpu
from jax.sharding import PartitionSpec as P

HQ = 6
HD = 128
SEC_T = 16
SEC_H = 24
BASE = 1000000.0
NEG = -1e30
F32 = jnp.float32
BF16 = jnp.bfloat16


def nt(a, b):
    return lax.dot_general(a, b, (((1,), (1,)), ((), ())), preferred_element_type=F32)


def nn(a, b):
    return lax.dot_general(a, b, (((1,), (0,)), ((), ())), preferred_element_type=F32)


def cos_turns(turns):
    r = turns - jnp.round(turns)
    b = 0.25 - jnp.abs(r)
    z = b * b
    acc = None
    for power in (11, 9, 7, 5, 3, 1):
        coef = (-1.0) ** ((power - 1) // 2) * (2.0 * math.pi) ** power / math.factorial(power)
        acc = jnp.full_like(z, coef) if acc is None else acc * z + coef
    return acc * b


def flip(me, i):
    out, bit = me, 1
    while bit <= i:
        if i & bit:
            out = out + bit - 2 * bit * ((me // bit) % 2)
        bit *= 2
    return out


def repeat(n, small, body):
    if small:
        for i in range(n):
            body(i)
    else:
        lax.fori_loop(0, n, lambda i, c: (body(i), c)[1], 0)


def kernel(n, order_ref, q_hbm, k_hbm, v_hbm, do_hbm, pos_hbm, doc_hbm,
           out_ref, gq_ref, gk_ref, gv_ref,
           q_in, do_in, pos_in, doc_in, k_all, v_all, feat, lay, seqtab, q_rot, do_st, krot,
           cos_t, sin_t, tops, s_buf, dp_buf, p_buf, ds_buf, send_buf, recv_buf,
           in_sem, ks_sem, kr_sem, vs_sem, vr_sem, gs_sem, gr_sem):
    me = lax.axis_index("cp")
    rows = k_hbm.shape[0]
    total = rows * n
    stretch = total // order_ref.shape[0]
    per = rows // stretch
    small = n <= 4 and n & (n - 1) == 0
    scale = 1.0 / math.sqrt(HD)
    mine = pl.ds(pl.multiple_of(me * rows, rows), rows)

    def to(i):
        return flip(me, i) if small else lax.rem(me + i, n)

    def frm(i):
        return flip(me, i) if small else lax.rem(me + n - i, n)

    def span(c):
        return pl.ds(pl.multiple_of(c * rows, rows), rows)

    loads = [
        pltpu.make_async_copy(src, dst, in_sem.at[j])
        for j, (src, dst) in enumerate((
            (k_hbm, k_all.at[mine]), (v_hbm, v_all.at[mine]), (pos_hbm, pos_in),
            (doc_hbm, doc_in), (q_hbm, q_in), (do_hbm, do_in)))
    ]
    for cp in loads:
        cp.start()

    barrier = pltpu.get_barrier_semaphore()

    def greet(i):
        pl.semaphore_signal(barrier, inc=1, device_id={"cp": to(i + 1)},
                            device_id_type=pl.DeviceIdType.MESH)

    repeat(n - 1, small, greet)
    loads[0].wait()
    loads[1].wait()
    pl.semaphore_wait(barrier, n - 1)

    def kcopy(i):
        return pltpu.make_async_remote_copy(
            src_ref=k_all.at[mine], dst_ref=k_all.at[mine], send_sem=ks_sem.at[i],
            recv_sem=kr_sem.at[i], device_id={"cp": to(i)}, device_id_type=pl.DeviceIdType.MESH)

    def vcopy(i):
        return pltpu.make_async_remote_copy(
            src_ref=v_all.at[mine], dst_ref=v_all.at[mine], send_sem=vs_sem.at[i],
            recv_sem=vr_sem.at[i], device_id={"cp": to(i)}, device_id_type=pl.DeviceIdType.MESH)

    repeat(n - 1, small, lambda i: kcopy(n - 1 - i).start())
    repeat(n - 1, small, lambda i: vcopy(n - 1 - i).start())

    for j in (2, 3):
        loads[j].wait()
    feat[...] = jnp.zeros_like(feat)
    feat[0:3, :] = pos_in[...].astype(F32)
    feat[3:4, :] = doc_in[...].astype(F32)
    tiles = [feat[:, t * rows:(t + 1) * rows] for t in range(n)]
    moved = [[tiles[t] if k == 0 else pltpu.roll(tiles[t], k * stretch, 1) for k in range(per)]
             for t in range(n)]
    lane8 = lax.broadcasted_iota(jnp.int32, (8, rows), 1)
    for t in range(n):
        whole = None
        for b in range(per):
            want = jnp.full((8, rows), order_ref[t * per + b], jnp.int32)
            acc = moved[0][b]
            for s in range(1, n * per):
                acc = jnp.where(want == s, moved[s // per][(b - s % per) % per], acc)
            whole = acc if b == 0 else jnp.where(lane8 >= b * stretch, acc, whole)
        lay[:, t * rows:(t + 1) * rows] = whole
    lane = lax.broadcasted_iota(jnp.int32, (8, 2 * HD), 1)
    row8 = lax.broadcasted_iota(jnp.int32, (8, 2 * HD), 0)
    pair = lane % (HD // 2)
    section = jnp.where(pair < SEC_T, 0, jnp.where(pair < SEC_T + SEC_H, 1, 2))
    freq = jnp.exp(pair.astype(F32) * (-2.0 / HD * math.log(BASE))) * (0.5 / math.pi)
    weights = jnp.where(lane < HD, jnp.where(row8 == section, freq, 0.0),
                        jnp.where(row8 == 3, 1.0, 0.0))
    seqtab[...] = lax.dot_general(lay[...], weights, (((0,), (0,)), ((), ())),
                                  precision=lax.Precision.HIGHEST, preferred_element_type=F32)

    first = lax.broadcasted_iota(jnp.int32, (rows, HD), 1) < HD // 2

    def blocks(c):
        return seqtab[span(c), :]

    def tables(turns):
        both = cos_turns(jnp.where(first, turns, turns - 0.25))
        other = pltpu.roll(both, HD // 2, 1)
        return jnp.where(first, both, other), jnp.where(first, -other, both)

    def turned(x):
        return pltpu.roll(x, HD // 2, 1)

    own = blocks(me)
    cosine, sine = tables(own[:, :HD])
    cos_t[...] = cosine
    sin_t[...] = sine
    r_idx = lax.broadcasted_iota(jnp.int32, (rows, HD), 0)
    l_idx = lax.broadcasted_iota(jnp.int32, (rows, HD), 1)
    doc_r = lay[3:4, mine]

    def places(c, idx):
        out = idx + order_ref[c * per] * stretch
        for b in range(1, per):
            out = jnp.where(idx >= b * stretch,
                            idx - b * stretch + order_ref[c * per + b] * stretch, out)
        return out

    orig_r = places(me, l_idx)

    loads[4].wait()
    loads[5].wait()
    for h in range(HQ):
        x = q_in[:, h * HD:(h + 1) * HD].astype(F32)
        q_rot[h * rows:(h + 1) * rows, :] = (x * cosine + turned(x) * sine).astype(BF16)
        do_st[h * rows:(h + 1) * rows, :] = do_in[:, h * HD:(h + 1) * HD]

    factor = scale * math.log2(math.e)

    def scores(c, tab, cc, ss):
        allowed = (tab[:, HD:] == doc_r) & (places(c, r_idx) <= orig_r)
        bias = jnp.where(allowed, 0.0, NEG)
        x = k_all[span(c), :].astype(F32)
        kr = (x * cc + turned(x) * ss).astype(BF16)
        krot[span(c), :] = kr
        sc = nt(kr, q_rot[...])
        peaks, sums = [], []
        for h in range(HQ):
            cols = slice(h * rows, (h + 1) * rows)
            part = sc[:, cols] + bias
            top = jnp.max(part, axis=0, keepdims=True)
            p = jnp.exp2((part - top) * factor)
            s_buf[span(c), cols] = p
            peaks.append(top)
            sums.append(jnp.sum(p, axis=0, keepdims=True))
        return jnp.concatenate(peaks, axis=1), jnp.concatenate(sums, axis=1)

    def grads(c):
        dp = nt(v_all[span(c), :], do_st[...])
        dp_buf[span(c), :] = dp
        return jnp.sum(s_buf[span(c), :] * dp, axis=0, keepdims=True)

    def merge(c, carry, top, total, weighted):
        m, l, d = carry
        tops[pl.ds(c, 1), :] = top
        new = jnp.maximum(m, top)
        old_w = jnp.exp2((m - new) * factor)
        new_w = jnp.exp2((top - new) * factor)
        return new, l * old_w + total * new_w, d * old_w + weighted * new_w

    top, total = scores(me, own, cosine, sine)
    weighted = grads(me)
    tops[pl.ds(me, 1), :] = top
    carry = (top, total, weighted)

    def arrive(i, carry):
        c = frm(i)
        tab = blocks(c)
        cc, ss = tables(tab[:, :HD])
        kcopy(i).wait_recv()
        top, total = scores(c, tab, cc, ss)
        vcopy(i).wait_recv()
        return merge(c, carry, top, total, grads(c))

    if small:
        for i in range(1, n):
            carry = arrive(i, carry)
    else:
        carry = lax.fori_loop(1, n, arrive, carry)
    inv = 1.0 / carry[1]
    delta = carry[2] * inv

    def back(c):
        share = jnp.exp2((tops[pl.ds(c, 1), :] - carry[0]) * factor) * inv
        probs = s_buf[span(c), :] * share
        pb = probs.astype(BF16)
        db = (probs * (dp_buf[span(c), :] - delta)).astype(BF16)
        p_buf[span(c), :] = pb
        ds_buf[span(c), :] = db
        return nn(db, q_rot[...]) * scale, nn(pb, do_st[...])

    def gcopy(i):
        return pltpu.make_async_remote_copy(
            src_ref=send_buf.at[i - 1], dst_ref=recv_buf.at[i - 1], send_sem=gs_sem.at[i],
            recv_sem=gr_sem.at[i], device_id={"cp": to(i)}, device_id_type=pl.DeviceIdType.MESH)

    def give(j):
        i = n - 1 - j
        dk, dv = back(to(i))
        send_buf[i - 1, :, :HD] = dk.astype(BF16)
        send_buf[i - 1, :, HD:] = dv.astype(BF16)
        gcopy(i).start()

    repeat(n - 1, small, give)
    dk, dv = back(me)

    outt = lax.dot_general(v_all[...], p_buf[...], (((0,), (0,)), ((), ())),
                           preferred_element_type=F32)
    dqt = lax.dot_general(krot[...], ds_buf[...], (((0,), (0,)), ((), ())),
                          preferred_element_type=F32) * scale
    for h in range(HQ):
        cols = slice(h * HD, (h + 1) * HD)
        out_ref[:, cols] = jnp.transpose(outt[:, h * rows:(h + 1) * rows]).astype(BF16)
        y = jnp.transpose(dqt[:, h * rows:(h + 1) * rows])
        gq_ref[:, cols] = (y * cos_t[...] - turned(y) * sin_t[...]).astype(BF16)

    def take(i, carry):
        gcopy(i).wait_recv()
        return (carry[0] + recv_buf[i - 1, :, :HD].astype(F32),
                carry[1] + recv_buf[i - 1, :, HD:].astype(F32))

    if small:
        for i in range(1, n):
            dk, dv = take(i, (dk, dv))
    else:
        dk, dv = lax.fori_loop(1, n, take, (dk, dv))
    gk_ref[...] = (dk * cos_t[...] - turned(dk) * sin_t[...]).astype(BF16)
    gv_ref[...] = dv.astype(BF16)

    def finish(j):
        kcopy(j + 1).wait_send()
        vcopy(j + 1).wait_send()
        gcopy(j + 1).wait_send()

    repeat(n - 1, small, finish)


def write_out(a, b, c, d, a_out, b_out, c_out, d_out, sem):
    copies = [
        pltpu.make_async_copy(src, dst, sem.at[j])
        for j, (src, dst) in enumerate(((a, a_out), (b, b_out), (c, c_out), (d, d_out)))
    ]
    for cp in copies:
        cp.start()
    for cp in copies:
        cp.wait()


def shards(queries, keys, values, out_grad, positions, doc_ids, stretch_order):
    n = lax.axis_size("cp")
    rows = queries.shape[0]
    total = rows * n
    wide = HQ * HD
    hbm = pl.BlockSpec(memory_space=pltpu.HBM)
    vmem = pl.BlockSpec(memory_space=pltpu.VMEM)
    dma = pltpu.SemaphoreType.DMA
    shapes = ((rows, wide), (rows, wide), (rows, HD), (rows, HD))
    held = pl.pallas_call(
        functools.partial(kernel, n),
        out_shape=tuple(pltpu.VMEM(shape, BF16) for shape in shapes),
        in_specs=[pl.BlockSpec(memory_space=pltpu.SMEM)] + [hbm] * 6,
        out_specs=(vmem,) * 4,
        scratch_shapes=[
            pltpu.VMEM((rows, wide), BF16),
            pltpu.VMEM((rows, wide), BF16),
            pltpu.VMEM((3, total), jnp.int32),
            pltpu.VMEM((1, total), jnp.int32),
            pltpu.VMEM((total, HD), BF16),
            pltpu.VMEM((total, HD), BF16),
            pltpu.VMEM((8, total), F32),
            pltpu.VMEM((8, total), F32),
            pltpu.VMEM((total, 2 * HD), F32),
            pltpu.VMEM((HQ * rows, HD), BF16),
            pltpu.VMEM((HQ * rows, HD), BF16),
            pltpu.VMEM((total, HD), BF16),
            pltpu.VMEM((rows, HD), F32),
            pltpu.VMEM((rows, HD), F32),
            pltpu.VMEM((n, HQ * rows), F32),
            pltpu.VMEM((total, HQ * rows), F32),
            pltpu.VMEM((total, HQ * rows), F32),
            pltpu.VMEM((total, HQ * rows), BF16),
            pltpu.VMEM((total, HQ * rows), BF16),
            pltpu.VMEM((n - 1, rows, 2 * HD), BF16),
            pltpu.VMEM((n - 1, rows, 2 * HD), BF16),
            dma((6,)),
            dma((n,)), dma((n,)), dma((n,)), dma((n,)), dma((n,)), dma((n,)),
        ],
        compiler_params=pltpu.CompilerParams(collective_id=0, has_side_effects=True),
    )(stretch_order, queries, keys, values, out_grad, positions, doc_ids[None, :])
    return pl.pallas_call(
        write_out,
        out_shape=tuple(jax.ShapeDtypeStruct(shape, BF16) for shape in shapes),
        in_specs=[vmem] * 4,
        out_specs=(hbm,) * 4,
        scratch_shapes=[dma((4,))],
    )(*[pltpu.with_memory_space_constraint(x, pltpu.VMEM) for x in held])


def solution(mesh):
    split = P(("seq", "cp"), None)
    return jax.shard_map(
        shards,
        mesh=mesh,
        in_specs=(split, split, split, split, P(None, "seq"), P("seq"), P("seq")),
        out_specs=(split, split, split, split),
        check_vma=False,
    )
```

```python
import functools
import math

import jax
import jax.numpy as jnp
from jax import lax
from jax.experimental import pallas as pl
from jax.experimental.pallas import tpu as pltpu
from jax.sharding import PartitionSpec as P

HQ = 6
HD = 128
SEC_T = 16
SEC_H = 24
BASE = 1000000.0
NEG = -1e30
F32 = jnp.float32
BF16 = jnp.bfloat16


def nt(a, b):
    return lax.dot_general(a, b, (((1,), (1,)), ((), ())), preferred_element_type=F32)


def nn(a, b):
    return lax.dot_general(a, b, (((1,), (0,)), ((), ())), preferred_element_type=F32)


def cos_turns(turns):
    r = turns - jnp.round(turns)
    b = 0.25 - jnp.abs(r)
    z = b * b
    acc = None
    for power in (11, 9, 7, 5, 3, 1):
        coef = (-1.0) ** ((power - 1) // 2) * (2.0 * math.pi) ** power / math.factorial(power)
        acc = jnp.full_like(z, coef) if acc is None else acc * z + coef
    return acc * b


def flip(me, i):
    out, bit = me, 1
    while bit <= i:
        if i & bit:
            out = out + bit - 2 * bit * ((me // bit) % 2)
        bit *= 2
    return out


def repeat(n, small, body):
    if small:
        for i in range(n):
            body(i)
    else:
        lax.fori_loop(0, n, lambda i, c: (body(i), c)[1], 0)


def kernel(n, order_ref, q_hbm, k_hbm, v_hbm, do_hbm, pos_hbm, doc_hbm,
           out_ref, gq_ref, gk_ref, gv_ref,
           q_in, do_in, pos_in, doc_in, k_all, v_all, feat, lay, seqtab, q_rot, do_st, krot,
           cos_t, sin_t, bias_t, tops, s_buf, dp_buf, p_buf, ds_buf, send_v, recv_v, send_k, recv_k,
           in_sem, ks_sem, kr_sem, vs_sem, vr_sem,
           gvs_sem, gvr_sem, gks_sem, gkr_sem):
    me = lax.axis_index("cp")
    rows = k_hbm.shape[0]
    total = rows * n
    stretch = total // order_ref.shape[0]
    per = rows // stretch
    small = n <= 4 and n & (n - 1) == 0
    scale = 1.0 / math.sqrt(HD)
    mine = pl.ds(pl.multiple_of(me * rows, rows), rows)

    def to(i):
        return flip(me, i) if small else lax.rem(me + i, n)

    def frm(i):
        return flip(me, i) if small else lax.rem(me + n - i, n)

    def span(c):
        return pl.ds(pl.multiple_of(c * rows, rows), rows)

    loads = [
        pltpu.make_async_copy(src, dst, in_sem.at[j])
        for j, (src, dst) in enumerate((
            (k_hbm, k_all.at[mine]), (v_hbm, v_all.at[mine]), (pos_hbm, pos_in),
            (doc_hbm, doc_in), (q_hbm, q_in), (do_hbm, do_in)))
    ]
    for cp in loads:
        cp.start()

    barrier = pltpu.get_barrier_semaphore()

    def greet(i):
        pl.semaphore_signal(barrier, inc=1, device_id={"cp": to(i + 1)},
                            device_id_type=pl.DeviceIdType.MESH)

    repeat(n - 1, small, greet)
    loads[0].wait()
    loads[1].wait()
    pl.semaphore_wait(barrier, n - 1)

    def kcopy(i):
        return pltpu.make_async_remote_copy(
            src_ref=k_all.at[mine], dst_ref=k_all.at[mine], send_sem=ks_sem.at[i],
            recv_sem=kr_sem.at[i], device_id={"cp": to(i)}, device_id_type=pl.DeviceIdType.MESH)

    def vcopy(i):
        return pltpu.make_async_remote_copy(
            src_ref=v_all.at[mine], dst_ref=v_all.at[mine], send_sem=vs_sem.at[i],
            recv_sem=vr_sem.at[i], device_id={"cp": to(i)}, device_id_type=pl.DeviceIdType.MESH)

    repeat(n - 1, small, lambda i: kcopy(n - 1 - i).start())
    repeat(n - 1, small, lambda i: vcopy(n - 1 - i).start())

    for j in (2, 3):
        loads[j].wait()
    feat[...] = jnp.zeros_like(feat)
    feat[0:3, :] = pos_in[...].astype(F32)
    feat[3:4, :] = doc_in[...].astype(F32)
    tiles = [feat[:, t * rows:(t + 1) * rows] for t in range(n)]
    moved = [[tiles[t] if k == 0 else pltpu.roll(tiles[t], k * stretch, 1) for k in range(per)]
             for t in range(n)]
    lane8 = lax.broadcasted_iota(jnp.int32, (8, rows), 1)
    for t in range(n):
        whole = None
        for b in range(per):
            want = jnp.full((8, rows), order_ref[t * per + b], jnp.int32)
            acc = moved[0][b]
            for s in range(1, n * per):
                acc = jnp.where(want == s, moved[s // per][(b - s % per) % per], acc)
            whole = acc if b == 0 else jnp.where(lane8 >= b * stretch, acc, whole)
        lay[:, t * rows:(t + 1) * rows] = whole
    lane = lax.broadcasted_iota(jnp.int32, (8, 2 * HD), 1)
    row8 = lax.broadcasted_iota(jnp.int32, (8, 2 * HD), 0)
    pair = lane % (HD // 2)
    section = jnp.where(pair < SEC_T, 0, jnp.where(pair < SEC_T + SEC_H, 1, 2))
    freq = jnp.exp(pair.astype(F32) * (-2.0 / HD * math.log(BASE))) * (0.5 / math.pi)
    weights = jnp.where(lane < HD, jnp.where(row8 == section, freq, 0.0),
                        jnp.where(row8 == 3, 1.0, 0.0))
    seqtab[...] = lax.dot_general(lay[...], weights, (((0,), (0,)), ((), ())),
                                  precision=lax.Precision.HIGHEST, preferred_element_type=F32)

    first = lax.broadcasted_iota(jnp.int32, (rows, HD), 1) < HD // 2

    def tables(turns):
        both = cos_turns(jnp.where(first, turns, turns - 0.25))
        other = pltpu.roll(both, HD // 2, 1)
        return jnp.where(first, both, other), jnp.where(first, -other, both)

    def turned(x):
        return pltpu.roll(x, HD // 2, 1)

    r_idx = lax.broadcasted_iota(jnp.int32, (rows, HD), 0)
    l_idx = lax.broadcasted_iota(jnp.int32, (rows, HD), 1)
    doc_r = lay[3:4, mine]

    def places(c, idx):
        out = idx + order_ref[c * per] * stretch
        for b in range(1, per):
            out = jnp.where(idx >= b * stretch,
                            idx - b * stretch + order_ref[c * per + b] * stretch, out)
        return out

    orig_r = places(me, l_idx)

    def prepare(c):
        tab = seqtab[span(c), :]
        cosine, sine = tables(tab[:, :HD])
        cos_t[span(c), :] = cosine
        sin_t[span(c), :] = sine
        allowed = (tab[:, HD:] == doc_r) & (places(c, r_idx) <= orig_r)
        bias_t[span(c), :] = jnp.where(allowed, 0.0, NEG)

    repeat(n, small, prepare)

    loads[4].wait()
    loads[5].wait()
    cosine = cos_t[mine, :]
    sine = sin_t[mine, :]
    for h in range(HQ):
        x = q_in[:, h * HD:(h + 1) * HD].astype(F32)
        q_rot[h * rows:(h + 1) * rows, :] = (x * cosine + turned(x) * sine).astype(BF16)
        do_st[h * rows:(h + 1) * rows, :] = do_in[:, h * HD:(h + 1) * HD]

    factor = scale * math.log2(math.e)

    def scores(c):
        x = k_all[span(c), :].astype(F32)
        kr = (x * cos_t[span(c), :] + turned(x) * sin_t[span(c), :]).astype(BF16)
        krot[span(c), :] = kr
        sc = nt(kr, q_rot[...])
        bias = bias_t[span(c), :]
        peaks, sums = [], []
        for h in range(HQ):
            cols = slice(h * rows, (h + 1) * rows)
            part = sc[:, cols] + bias
            top = jnp.max(part, axis=0, keepdims=True)
            p = jnp.exp2((part - top) * factor)
            s_buf[span(c), cols] = p
            peaks.append(top)
            sums.append(jnp.sum(p, axis=0, keepdims=True))
        top = jnp.concatenate(peaks, axis=1)
        tops[pl.ds(c, 1), :] = top
        return top, jnp.concatenate(sums, axis=1)

    def arrive(i, carry):
        c = frm(i)
        kcopy(i).wait_recv()
        m, l = carry
        top, total = scores(c)
        new = jnp.maximum(m, top)
        return new, l * jnp.exp2((m - new) * factor) + total * jnp.exp2((top - new) * factor)

    carry = scores(me)
    dp_buf[mine, :] = nt(v_all[mine, :], do_st[...])
    if small:
        for i in range(1, n):
            carry = arrive(i, carry)
    else:
        carry = lax.fori_loop(1, n, arrive, carry)
    top = carry[0]
    inv = 1.0 / carry[1]

    def value_grad(c):
        probs = s_buf[span(c), :] * (jnp.exp2((tops[pl.ds(c, 1), :] - top) * factor) * inv)
        pb = probs.astype(BF16)
        s_buf[span(c), :] = probs
        p_buf[span(c), :] = pb
        return nn(pb, do_st[...])

    def gvcopy(i):
        return pltpu.make_async_remote_copy(
            src_ref=send_v.at[i - 1], dst_ref=recv_v.at[i - 1], send_sem=gvs_sem.at[i],
            recv_sem=gvr_sem.at[i], device_id={"cp": to(i)}, device_id_type=pl.DeviceIdType.MESH)

    def gkcopy(i):
        return pltpu.make_async_remote_copy(
            src_ref=send_k.at[i - 1], dst_ref=recv_k.at[i - 1], send_sem=gks_sem.at[i],
            recv_sem=gkr_sem.at[i], device_id={"cp": to(i)}, device_id_type=pl.DeviceIdType.MESH)

    def give_v(j):
        i = n - 1 - j
        send_v[i - 1, :, :] = value_grad(to(i)).astype(BF16)
        gvcopy(i).start()

    repeat(n - 1, small, give_v)
    dv = value_grad(me)
    delta = jnp.sum(s_buf[mine, :] * dp_buf[mine, :], axis=0, keepdims=True)

    def weigh(i, delta):
        c = frm(i)
        vcopy(i).wait_recv()
        dp = nt(v_all[span(c), :], do_st[...])
        dp_buf[span(c), :] = dp
        return delta + jnp.sum(s_buf[span(c), :] * dp, axis=0, keepdims=True)

    if small:
        for i in range(1, n):
            delta = weigh(i, delta)
    else:
        delta = lax.fori_loop(1, n, weigh, delta)

    def key_grad(c):
        db = (s_buf[span(c), :] * (dp_buf[span(c), :] - delta)).astype(BF16)
        ds_buf[span(c), :] = db
        return nn(db, q_rot[...]) * scale

    def give_k(j):
        i = n - 1 - j
        send_k[i - 1, :, :] = key_grad(to(i)).astype(BF16)
        gkcopy(i).start()

    repeat(n - 1, small, give_k)
    dk = key_grad(me)

    outt = lax.dot_general(v_all[...], p_buf[...], (((0,), (0,)), ((), ())),
                           preferred_element_type=F32)
    dqt = lax.dot_general(krot[...], ds_buf[...], (((0,), (0,)), ((), ())),
                          preferred_element_type=F32) * scale
    for h in range(HQ):
        cols = slice(h * HD, (h + 1) * HD)
        out_ref[:, cols] = jnp.transpose(outt[:, h * rows:(h + 1) * rows]).astype(BF16)
        y = jnp.transpose(dqt[:, h * rows:(h + 1) * rows])
        gq_ref[:, cols] = (y * cosine - turned(y) * sine).astype(BF16)

    def take_v(i, dv):
        gvcopy(i).wait_recv()
        return dv + recv_v[i - 1, :, :].astype(F32)

    def take_k(i, dk):
        gkcopy(i).wait_recv()
        return dk + recv_k[i - 1, :, :].astype(F32)

    if small:
        for i in range(1, n):
            dv = take_v(i, dv)
        gv_ref[...] = dv.astype(BF16)
        for i in range(1, n):
            dk = take_k(i, dk)
    else:
        gv_ref[...] = lax.fori_loop(1, n, take_v, dv).astype(BF16)
        dk = lax.fori_loop(1, n, take_k, dk)
    gk_ref[...] = (dk * cosine - turned(dk) * sine).astype(BF16)

    def finish(j):
        kcopy(j + 1).wait_send()
        vcopy(j + 1).wait_send()
        gvcopy(j + 1).wait_send()
        gkcopy(j + 1).wait_send()

    repeat(n - 1, small, finish)


def write_out(a, b, c, d, a_out, b_out, c_out, d_out, sem):
    copies = [
        pltpu.make_async_copy(src, dst, sem.at[j])
        for j, (src, dst) in enumerate(((a, a_out), (b, b_out), (c, c_out), (d, d_out)))
    ]
    for cp in copies:
        cp.start()
    for cp in copies:
        cp.wait()


def shards(queries, keys, values, out_grad, positions, doc_ids, stretch_order):
    n = lax.axis_size("cp")
    rows = queries.shape[0]
    total = rows * n
    wide = HQ * HD
    hbm = pl.BlockSpec(memory_space=pltpu.HBM)
    vmem = pl.BlockSpec(memory_space=pltpu.VMEM)
    dma = pltpu.SemaphoreType.DMA
    shapes = ((rows, wide), (rows, wide), (rows, HD), (rows, HD))
    held = pl.pallas_call(
        functools.partial(kernel, n),
        out_shape=tuple(pltpu.VMEM(shape, BF16) for shape in shapes),
        in_specs=[pl.BlockSpec(memory_space=pltpu.SMEM)] + [hbm] * 6,
        out_specs=(vmem,) * 4,
        scratch_shapes=[
            pltpu.VMEM((rows, wide), BF16),
            pltpu.VMEM((rows, wide), BF16),
            pltpu.VMEM((3, total), jnp.int32),
            pltpu.VMEM((1, total), jnp.int32),
            pltpu.VMEM((total, HD), BF16),
            pltpu.VMEM((total, HD), BF16),
            pltpu.VMEM((8, total), F32),
            pltpu.VMEM((8, total), F32),
            pltpu.VMEM((total, 2 * HD), F32),
            pltpu.VMEM((HQ * rows, HD), BF16),
            pltpu.VMEM((HQ * rows, HD), BF16),
            pltpu.VMEM((total, HD), BF16),
            pltpu.VMEM((total, HD), F32),
            pltpu.VMEM((total, HD), F32),
            pltpu.VMEM((total, rows), F32),
            pltpu.VMEM((n, HQ * rows), F32),
            pltpu.VMEM((total, HQ * rows), F32),
            pltpu.VMEM((total, HQ * rows), F32),
            pltpu.VMEM((total, HQ * rows), BF16),
            pltpu.VMEM((total, HQ * rows), BF16),
            pltpu.VMEM((n - 1, rows, HD), BF16),
            pltpu.VMEM((n - 1, rows, HD), BF16),
            pltpu.VMEM((n - 1, rows, HD), BF16),
            pltpu.VMEM((n - 1, rows, HD), BF16),
            dma((6,)),
            dma((n,)), dma((n,)), dma((n,)), dma((n,)), dma((n,)), dma((n,)), dma((n,)), dma((n,)),
        ],
        compiler_params=pltpu.CompilerParams(collective_id=0, has_side_effects=True),
    )(stretch_order, queries, keys, values, out_grad, positions, doc_ids[None, :])
    return pl.pallas_call(
        write_out,
        out_shape=tuple(jax.ShapeDtypeStruct(shape, BF16) for shape in shapes),
        in_specs=[vmem] * 4,
        out_specs=(hbm,) * 4,
        scratch_shapes=[dma((4,))],
    )(*[pltpu.with_memory_space_constraint(x, pltpu.VMEM) for x in held])


def solution(mesh):
    split = P(("seq", "cp"), None)
    return jax.shard_map(
        shards,
        mesh=mesh,
        in_specs=(split, split, split, split, P(None, "seq"), P("seq"), P("seq")),
        out_specs=(split, split, split, split),
        check_vma=False,
    )
```

```python
import functools
import math

import jax
import jax.numpy as jnp
from jax import lax
from jax.experimental import pallas as pl
from jax.experimental.pallas import tpu as pltpu
from jax.sharding import PartitionSpec as P

HQ = 6
HD = 128
SEC_T = 16
SEC_H = 24
BASE = 1000000.0
NEG = -1e30
F32 = jnp.float32
BF16 = jnp.bfloat16


def nt(a, b):
    return lax.dot_general(a, b, (((1,), (1,)), ((), ())), preferred_element_type=F32)


def nn(a, b):
    return lax.dot_general(a, b, (((1,), (0,)), ((), ())), preferred_element_type=F32)


def cos_turns(turns):
    r = turns - jnp.round(turns)
    b = 0.25 - jnp.abs(r)
    z = b * b
    acc = None
    for power in (11, 9, 7, 5, 3, 1):
        coef = (-1.0) ** ((power - 1) // 2) * (2.0 * math.pi) ** power / math.factorial(power)
        acc = jnp.full_like(z, coef) if acc is None else acc * z + coef
    return acc * b


def flip(me, i):
    out, bit = me, 1
    while bit <= i:
        if i & bit:
            out = out + bit - 2 * bit * ((me // bit) % 2)
        bit *= 2
    return out


def repeat(n, small, body):
    if small:
        for i in range(n):
            body(i)
    else:
        lax.fori_loop(0, n, lambda i, c: (body(i), c)[1], 0)


def kernel(n, order_hbm, q_hbm, k_hbm, v_hbm, do_hbm, pos_hbm, doc_hbm,
           out_ref, gq_ref, gk_ref, gv_ref,
           order_ref, q_in, do_in, pos_in, doc_in, k_all, v_all, feat, lay, seqtab, q_rot, do_st, krot,
           cos_t, sin_t, bias_t, tops, s_buf, dp_buf, p_buf, ds_buf, send_v, recv_v, send_k, recv_k,
           in_sem, ks_sem, kr_sem, vs_sem, vr_sem,
           gvs_sem, gvr_sem, gks_sem, gkr_sem):
    me = lax.axis_index("cp")
    rows = k_hbm.shape[0]
    total = rows * n
    stretch = total // order_hbm.shape[0]
    per = rows // stretch
    small = n <= 4 and n & (n - 1) == 0
    scale = 1.0 / math.sqrt(HD)
    mine = pl.ds(pl.multiple_of(me * rows, rows), rows)

    def to(i):
        return flip(me, i) if small else lax.rem(me + i, n)

    def frm(i):
        return flip(me, i) if small else lax.rem(me + n - i, n)

    def span(c):
        return pl.ds(pl.multiple_of(c * rows, rows), rows)

    barrier = pltpu.get_barrier_semaphore()

    def greet(i):
        pl.semaphore_signal(barrier, inc=1, device_id={"cp": to(n - 1 - i)},
                            device_id_type=pl.DeviceIdType.MESH)

    repeat(n - 1, small, greet)

    loads = [
        pltpu.make_async_copy(src, dst, in_sem.at[j])
        for j, (src, dst) in enumerate((
            (k_hbm, k_all.at[mine]), (v_hbm, v_all.at[mine]), (pos_hbm, pos_in),
            (doc_hbm, doc_in), (q_hbm, q_in), (do_hbm, do_in), (order_hbm, order_ref)))
    ]
    for cp in loads:
        cp.start()

    loads[0].wait()
    loads[1].wait()
    pl.semaphore_wait(barrier, n - 1)

    def kcopy(i):
        return pltpu.make_async_remote_copy(
            src_ref=k_all.at[mine], dst_ref=k_all.at[mine], send_sem=ks_sem.at[i],
            recv_sem=kr_sem.at[i], device_id={"cp": to(i)}, device_id_type=pl.DeviceIdType.MESH)

    def vcopy(i):
        return pltpu.make_async_remote_copy(
            src_ref=v_all.at[mine], dst_ref=v_all.at[mine], send_sem=vs_sem.at[i],
            recv_sem=vr_sem.at[i], device_id={"cp": to(i)}, device_id_type=pl.DeviceIdType.MESH)

    repeat(n - 1, small, lambda i: kcopy(n - 1 - i).start())
    repeat(n - 1, small, lambda i: vcopy(n - 1 - i).start())

    for j in (2, 3, 6):
        loads[j].wait()
    feat[...] = jnp.zeros_like(feat)
    feat[0:3, :] = pos_in[...].astype(F32)
    feat[3:4, :] = doc_in[...].astype(F32)
    tiles = [feat[:, t * rows:(t + 1) * rows] for t in range(n)]
    moved = [[tiles[t] if k == 0 else pltpu.roll(tiles[t], k * stretch, 1) for k in range(per)]
             for t in range(n)]
    lane8 = lax.broadcasted_iota(jnp.int32, (8, rows), 1)
    for t in range(n):
        whole = None
        for b in range(per):
            want = jnp.full((8, rows), order_ref[t * per + b], jnp.int32)
            acc = moved[0][b]
            for s in range(1, n * per):
                acc = jnp.where(want == s, moved[s // per][(b - s % per) % per], acc)
            whole = acc if b == 0 else jnp.where(lane8 >= b * stretch, acc, whole)
        lay[:, t * rows:(t + 1) * rows] = whole
    lane = lax.broadcasted_iota(jnp.int32, (8, 2 * HD), 1)
    row8 = lax.broadcasted_iota(jnp.int32, (8, 2 * HD), 0)
    pair = lane % (HD // 2)
    section = jnp.where(pair < SEC_T, 0, jnp.where(pair < SEC_T + SEC_H, 1, 2))
    freq = jnp.exp(pair.astype(F32) * (-2.0 / HD * math.log(BASE))) * (0.5 / math.pi)
    weights = jnp.where(lane < HD, jnp.where(row8 == section, freq, 0.0),
                        jnp.where(row8 == 3, 1.0, 0.0))
    seqtab[...] = lax.dot_general(lay[...], weights, (((0,), (0,)), ((), ())),
                                  precision=lax.Precision.HIGHEST, preferred_element_type=F32)

    first = lax.broadcasted_iota(jnp.int32, (rows, HD), 1) < HD // 2

    def tables(turns):
        both = cos_turns(jnp.where(first, turns, turns - 0.25))
        other = pltpu.roll(both, HD // 2, 1)
        return jnp.where(first, both, other), jnp.where(first, -other, both)

    def turned(x):
        return pltpu.roll(x, HD // 2, 1)

    r_idx = lax.broadcasted_iota(jnp.int32, (rows, HD), 0)
    l_idx = lax.broadcasted_iota(jnp.int32, (rows, HD), 1)
    doc_r = lay[3:4, mine]

    def places(c, idx):
        out = idx + order_ref[c * per] * stretch
        for b in range(1, per):
            out = jnp.where(idx >= b * stretch,
                            idx - b * stretch + order_ref[c * per + b] * stretch, out)
        return out

    orig_r = places(me, l_idx)

    def prepare(c):
        tab = seqtab[span(c), :]
        cosine, sine = tables(tab[:, :HD])
        cos_t[span(c), :] = cosine
        sin_t[span(c), :] = sine
        allowed = (tab[:, HD:] == doc_r) & (places(c, r_idx) <= orig_r)
        bias_t[span(c), :] = jnp.where(allowed, 0.0, NEG)

    repeat(n, small, prepare)

    loads[4].wait()
    loads[5].wait()
    cosine = cos_t[mine, :]
    sine = sin_t[mine, :]
    for h in range(HQ):
        x = q_in[:, h * HD:(h + 1) * HD].astype(F32)
        q_rot[h * rows:(h + 1) * rows, :] = (x * cosine + turned(x) * sine).astype(BF16)
        do_st[h * rows:(h + 1) * rows, :] = do_in[:, h * HD:(h + 1) * HD]

    factor = scale * math.log2(math.e)

    def scores(c):
        x = k_all[span(c), :].astype(F32)
        kr = (x * cos_t[span(c), :] + turned(x) * sin_t[span(c), :]).astype(BF16)
        krot[span(c), :] = kr
        sc = nt(kr, q_rot[...])
        bias = bias_t[span(c), :]
        peaks, sums = [], []
        for h in range(HQ):
            cols = slice(h * rows, (h + 1) * rows)
            part = sc[:, cols] + bias
            top = jnp.max(part, axis=0, keepdims=True)
            p = jnp.exp2((part - top) * factor)
            s_buf[span(c), cols] = p
            peaks.append(top)
            sums.append(jnp.sum(p, axis=0, keepdims=True))
        top = jnp.concatenate(peaks, axis=1)
        tops[pl.ds(c, 1), :] = top
        return top, jnp.concatenate(sums, axis=1)

    def arrive(i, carry):
        c = frm(i)
        kcopy(i).wait_recv()
        m, l = carry
        top, total = scores(c)
        new = jnp.maximum(m, top)
        return new, l * jnp.exp2((m - new) * factor) + total * jnp.exp2((top - new) * factor)

    carry = scores(me)
    dp_buf[mine, :] = nt(v_all[mine, :], do_st[...])
    if small:
        for i in range(1, n):
            carry = arrive(i, carry)
    else:
        carry = lax.fori_loop(1, n, arrive, carry)
    top = carry[0]
    inv = 1.0 / carry[1]

    def value_grad(c):
        probs = s_buf[span(c), :] * (jnp.exp2((tops[pl.ds(c, 1), :] - top) * factor) * inv)
        pb = probs.astype(BF16)
        s_buf[span(c), :] = probs
        p_buf[span(c), :] = pb
        return nn(pb, do_st[...])

    def gvcopy(i):
        return pltpu.make_async_remote_copy(
            src_ref=send_v.at[i - 1], dst_ref=recv_v.at[i - 1], send_sem=gvs_sem.at[i],
            recv_sem=gvr_sem.at[i], device_id={"cp": to(i)}, device_id_type=pl.DeviceIdType.MESH)

    def gkcopy(i):
        return pltpu.make_async_remote_copy(
            src_ref=send_k.at[i - 1], dst_ref=recv_k.at[i - 1], send_sem=gks_sem.at[i],
            recv_sem=gkr_sem.at[i], device_id={"cp": to(i)}, device_id_type=pl.DeviceIdType.MESH)

    def give_v(j):
        i = n - 1 - j
        send_v[i - 1, :, :] = value_grad(to(i)).astype(BF16)
        gvcopy(i).start()

    repeat(n - 1, small, give_v)
    dv = value_grad(me)
    delta = jnp.sum(s_buf[mine, :] * dp_buf[mine, :], axis=0, keepdims=True)

    def weigh(i, delta):
        c = frm(i)
        vcopy(i).wait_recv()
        dp = nt(v_all[span(c), :], do_st[...])
        dp_buf[span(c), :] = dp
        return delta + jnp.sum(s_buf[span(c), :] * dp, axis=0, keepdims=True)

    if small:
        for i in range(1, n):
            delta = weigh(i, delta)
    else:
        delta = lax.fori_loop(1, n, weigh, delta)

    def key_grad(c):
        db = (s_buf[span(c), :] * (dp_buf[span(c), :] - delta)).astype(BF16)
        ds_buf[span(c), :] = db
        return nn(db, q_rot[...]) * scale

    def give_k(j):
        i = n - 1 - j
        send_k[i - 1, :, :] = key_grad(to(i)).astype(BF16)
        gkcopy(i).start()

    repeat(n - 1, small, give_k)
    dk = key_grad(me)

    outt = lax.dot_general(v_all[...], p_buf[...], (((0,), (0,)), ((), ())),
                           preferred_element_type=F32)
    dqt = lax.dot_general(krot[...], ds_buf[...], (((0,), (0,)), ((), ())),
                          preferred_element_type=F32) * scale
    for h in range(HQ):
        cols = slice(h * HD, (h + 1) * HD)
        out_ref[:, cols] = jnp.transpose(outt[:, h * rows:(h + 1) * rows]).astype(BF16)
        y = jnp.transpose(dqt[:, h * rows:(h + 1) * rows])
        gq_ref[:, cols] = (y * cosine - turned(y) * sine).astype(BF16)

    def take_v(i, dv):
        gvcopy(i).wait_recv()
        return dv + recv_v[i - 1, :, :].astype(F32)

    def take_k(i, dk):
        gkcopy(i).wait_recv()
        return dk + recv_k[i - 1, :, :].astype(F32)

    if small:
        for i in range(1, n):
            dv = take_v(i, dv)
        gv_ref[...] = dv.astype(BF16)
        for i in range(1, n):
            dk = take_k(i, dk)
    else:
        gv_ref[...] = lax.fori_loop(1, n, take_v, dv).astype(BF16)
        dk = lax.fori_loop(1, n, take_k, dk)
    gk_ref[...] = (dk * cosine - turned(dk) * sine).astype(BF16)

    def finish(j):
        kcopy(j + 1).wait_send()
        vcopy(j + 1).wait_send()
        gvcopy(j + 1).wait_send()
        gkcopy(j + 1).wait_send()

    repeat(n - 1, small, finish)


def write_out(a, b, c, d, a_out, b_out, c_out, d_out, sem):
    copies = [
        pltpu.make_async_copy(src, dst, sem.at[j])
        for j, (src, dst) in enumerate(((a, a_out), (b, b_out), (c, c_out), (d, d_out)))
    ]
    for cp in copies:
        cp.start()
    for cp in copies:
        cp.wait()


def shards(queries, keys, values, out_grad, positions, doc_ids, stretch_order):
    n = lax.axis_size("cp")
    rows = queries.shape[0]
    total = rows * n
    wide = HQ * HD
    hbm = pl.BlockSpec(memory_space=pltpu.HBM)
    vmem = pl.BlockSpec(memory_space=pltpu.VMEM)
    dma = pltpu.SemaphoreType.DMA
    shapes = ((rows, wide), (rows, wide), (rows, HD), (rows, HD))
    held = pl.pallas_call(
        functools.partial(kernel, n),
        out_shape=tuple(pltpu.VMEM(shape, BF16) for shape in shapes),
        in_specs=[hbm] * 7,
        out_specs=(vmem,) * 4,
        scratch_shapes=[
            pltpu.SMEM(stretch_order.shape, jnp.int32),
            pltpu.VMEM((rows, wide), BF16),
            pltpu.VMEM((rows, wide), BF16),
            pltpu.VMEM((3, total), jnp.int32),
            pltpu.VMEM((1, total), jnp.int32),
            pltpu.VMEM((total, HD), BF16),
            pltpu.VMEM((total, HD), BF16),
            pltpu.VMEM((8, total), F32),
            pltpu.VMEM((8, total), F32),
            pltpu.VMEM((total, 2 * HD), F32),
            pltpu.VMEM((HQ * rows, HD), BF16),
            pltpu.VMEM((HQ * rows, HD), BF16),
            pltpu.VMEM((total, HD), BF16),
            pltpu.VMEM((total, HD), F32),
            pltpu.VMEM((total, HD), F32),
            pltpu.VMEM((total, rows), F32),
            pltpu.VMEM((n, HQ * rows), F32),
            pltpu.VMEM((total, HQ * rows), F32),
            pltpu.VMEM((total, HQ * rows), F32),
            pltpu.VMEM((total, HQ * rows), BF16),
            pltpu.VMEM((total, HQ * rows), BF16),
            pltpu.VMEM((n - 1, rows, HD), BF16),
            pltpu.VMEM((n - 1, rows, HD), BF16),
            pltpu.VMEM((n - 1, rows, HD), BF16),
            pltpu.VMEM((n - 1, rows, HD), BF16),
            dma((7,)),
            dma((n,)), dma((n,)), dma((n,)), dma((n,)), dma((n,)), dma((n,)), dma((n,)), dma((n,)),
        ],
        compiler_params=pltpu.CompilerParams(collective_id=0, has_side_effects=True),
    )(stretch_order, queries, keys, values, out_grad, positions, doc_ids[None, :])
    return pl.pallas_call(
        write_out,
        out_shape=tuple(jax.ShapeDtypeStruct(shape, BF16) for shape in shapes),
        in_specs=[vmem] * 4,
        out_specs=(hbm,) * 4,
        scratch_shapes=[dma((4,))],
    )(*[pltpu.with_memory_space_constraint(x, pltpu.VMEM) for x in held])


def solution(mesh):
    split = P(("seq", "cp"), None)
    return jax.shard_map(
        shards,
        mesh=mesh,
        in_specs=(split, split, split, split, P(None, "seq"), P("seq"), P("seq")),
        out_specs=(split, split, split, split),
        check_vma=False,
    )
```
